256 devices in a mesh: fsdp: 64 (over z, x, core), tp: 4 (over y).
Axes of the slice: x: 4, y: 4, z: 8, core: 2. Of those that a mesh axis runs over, the one named last changes fastest.
Arguments:
- slopes_in: float32 [256, 128, 4096], P(None, 'fsdp', 'tp'), may hold values from -6 to 6
- moments_in: float32 [256, 128, 4096], P(None, 'fsdp', 'tp'), may hold values from -6 to 6
- weights_in: float32 [256, 128, 4096], P(None, 'fsdp', 'tp'), may hold values from -0.1875 to 0.1875
Outputs:
- new_weights: float32 [256, 128, 4096], P(None, 'fsdp', 'tp')
- new_momentum: float32 [256, 128, 4096], P(None, 'fsdp', 'tp')
The draws below stay inside these ranges and needn't reach their ends.
All inputs are finite; a program needn't handle non-finite values.
Results may differ from the reference program's by a relative error of at most 0.00021.
Values sent between devices are 32-bit elements; how exact they have to be, the bound alone decides.
A program may use at most 128 MiB of HBM per device.

```python
import jax
import jax.numpy as jnp
from jax import lax

SIDE = 128
WIDE = 4096
MATS = 256
ITERS = 5


def level_of(own_key, dims, split, smallest, top_value):
    level, own = 1.0, jax.random.fold_in(own_key, 6)
    for position, parts in split:
        heights = jnp.exp(jax.random.uniform(jax.random.fold_in(own, position), (parts,), jnp.float32, smallest / len(split), top_value / len(split)))
        level = level * jnp.repeat(heights, dims[position] // parts).reshape([-1 if axis == position else 1 for axis in range(len(dims))])
    return level


def normal_values(key, extent, scale, reach, cuts=(), held_as=jnp.bfloat16):
    loudness = level_of(key, extent, cuts, -0.22, 0.18) if cuts else 1.0
    array = jax.random.normal(key, extent, jnp.float32) * scale * loudness
    return jnp.minimum(jnp.maximum(array, -reach), reach).astype(held_as)


def setup_inputs(seed: int = 0) -> dict:
    seeds = jax.random.split(jax.random.key(seed), 4)
    slopes_in = normal_values(seeds[0], (MATS, SIDE, WIDE), 1.0, 6.0, ((1, 64), (2, 4)), jnp.float32)
    moments_in = normal_values(seeds[1], (MATS, SIDE, WIDE), 1.0, 6.0, ((1, 64), (2, 4)), jnp.float32)
    weights_in = normal_values(seeds[2], (MATS, SIDE, WIDE), 0.03, 0.1875, ((1, 64), (2, 4)), jnp.float32)
    return {"slopes_in": slopes_in, "moments_in": moments_in, "weights_in": weights_in}


hold_rate = 0.8
learn_rate = 1.0

def reference(slopes_in, moments_in, weights_in):
    new_momentum = hold_rate * moments_in + slopes_in

    def orthogonal_one(stack):
        iterate = stack[None]
        iterate = iterate * lax.rsqrt(lax.optimization_barrier(jnp.sum(iterate * iterate, axis=(1, 2), keepdims=True)) + 1e-06)
        for step in range(ITERS):
            gram = jnp.einsum('mik,mjk->mij', iterate, iterate, precision=lax.Precision.HIGHEST)
            mixed = -4.775 * gram + 2.0315 * jnp.einsum('mij,mjk->mik', gram, gram, precision=lax.Precision.HIGHEST)
            iterate = 3.4445 * iterate + jnp.einsum('mij,mjk->mik', mixed, iterate, precision=lax.Precision.HIGHEST)
        return iterate[0]
    iterate = lax.map(orthogonal_one, new_momentum)
    new_weights = weights_in - learn_rate * iterate
    return (new_weights, new_momentum)
```

```python
import jax
import jax.numpy as jnp
from jax import lax
from jax.experimental import pallas as pl
from jax.experimental.pallas import tpu as pltpu
from jax.sharding import PartitionSpec as P

HOLD = 0.8
RATE = 1.0
CA, CB, CC = 3.4445, -4.775, 2.0315
LANES = 128
SIDE = 128
MESH = pl.DeviceIdType.MESH


def dot(a, b, contract=0):
    return lax.dot_general(
        a,
        b,
        (((1,), (contract,)), ((), ())),
        precision=lax.Precision.HIGHEST,
        preferred_element_type=jnp.float32,
    )


def eye():
    shape = (SIDE, SIDE)
    rows = lax.broadcasted_iota(jnp.int32, shape, 0)
    return (rows == lax.broadcasted_iota(jnp.int32, shape, 1)).astype(jnp.float32)


def poly(gram, one):
    return CA * one + CB * gram + CC * dot(gram, gram)


def three_steps(gram, one):
    scale = lax.rsqrt(jnp.sum(gram * one) + 1e-06)
    gram = gram * (scale * scale)
    first = poly(gram, one)
    gram = dot(dot(first, gram), first)
    second = poly(gram, one)
    both = dot(second, first)
    gram = dot(dot(second, gram), second)
    return dot(poly(gram, one), both) * scale


def two_steps(gram, one):
    first = poly(gram, one)
    gram = dot(dot(first, gram), first)
    return dot(poly(gram, one), first)


def make_kernel(fs, tp, mats, wide):
    chunks = mats // fs
    span = 2 * wide // LANES
    cols = wide // LANES
    part = fs * span
    others = fs - 1

    def kernel(
        slopes, moments, weights, new_w, new_m,
        s_buf, m_buf, recv, res, back, w_buf, x_buf, x3_buf, grams,
        s_sem, m_sem, w_sem, f_send, f_recv, b_send, b_recv, g_send, g_recv,
    ):
        me = lax.axis_index("fsdp")
        col = lax.axis_index("tp")
        z, x, c = me // 8, (me // 2) % 4, me % 2

        def peer(i):
            far, near = i // 8, i % 8
            up = (far + 1) // 2
            step = (far % 2) * up + (1 - far % 2) * (8 - far // 2)
            return ((z + step) % 8) * 8 + ((x + near // 2) % 4) * 2 + (c + near % 2) % 2

        def chunk(k):
            return pl.ds(pl.multiple_of(k * part, part), part)

        def block(k, j):
            return pl.ds(pl.multiple_of(k * part + j * span, span), span)

        def load(k):
            pltpu.make_async_copy(slopes.at[chunk(k)], s_buf.at[chunk(k)], s_sem.at[k]).start()
            pltpu.make_async_copy(moments.at[chunk(k)], m_buf.at[chunk(k)], m_sem.at[k]).start()

        def send(src, dst, k, i, send_sem, recv_sem):
            j = peer(i)
            pltpu.make_async_remote_copy(
                src_ref=src.at[block(k, j)],
                dst_ref=dst.at[block(k, me)],
                send_sem=send_sem,
                recv_sem=recv_sem.at[k],
                device_id=(j, col),
                device_id_type=MESH,
            ).start()

        def send_all(src, dst, k, send_sem, recv_sem):
            def go(i, carry):
                send(src, dst, k, i, send_sem, recv_sem)
                return carry

            lax.fori_loop(1, fs, go, 0)

        def wait_rows(buf, n, sem):
            rows = pl.ds(0, n * span)
            pltpu.make_async_copy(buf.at[rows], buf.at[rows], sem).wait()

        load(0)
        barrier = pltpu.get_barrier_semaphore()

        def greet(i, carry):
            pl.semaphore_signal(barrier, inc=1, device_id=(peer(i), col), device_id_type=MESH)
            return carry

        lax.fori_loop(1, fs, greet, 0)
        for d in range(1, tp):
            pl.semaphore_signal(barrier, inc=1, device_id=(me, (col + d) % tp), device_id_type=MESH)
        for k in range(1, chunks):
            load(k)
        pltpu.make_async_copy(weights, w_buf, w_sem).start()

        def momentum(k, carry):
            pltpu.make_async_copy(slopes.at[chunk(k)], s_buf.at[chunk(k)], s_sem.at[k]).wait()
            pltpu.make_async_copy(moments.at[chunk(k)], m_buf.at[chunk(k)], m_sem.at[k]).wait()
            new_m[chunk(k), :] = HOLD * m_buf[chunk(k), :] + s_buf[chunk(k), :]
            return carry

        momentum(0, 0)
        pl.semaphore_wait(barrier, others + tp - 1)

        def spread(k, carry):
            send_all(new_m, recv, k, f_send, f_recv)
            recv[block(k, me), :] = new_m[block(k, me), :]
            return carry

        spread(0, 0)

        def rest(k, carry):
            momentum(k, 0)
            return spread(k, 0)

        lax.fori_loop(1, chunks, rest, 0)

        one = eye()

        def share(turn, k, value):
            grams[turn, k, col] = value
            copies = []
            for d in range(1, tp):
                copies.append(
                    pltpu.make_async_remote_copy(
                        src_ref=grams.at[turn, k, col],
                        dst_ref=grams.at[turn, k, col],
                        send_sem=g_send.at[turn, d - 1],
                        recv_sem=g_recv.at[turn, k, d - 1],
                        device_id=(me, (col + d) % tp),
                        device_id_type=MESH,
                    )
                )
            for copy in copies:
                copy.start()
            for copy in copies:
                copy.wait()
            total = grams[turn, k, 0]
            for t in range(1, tp):
                total = total + grams[turn, k, t]
            return total

        def work(k, carry):
            wait_rows(recv, others, f_recv.at[k])
            for t in range(cols):
                for r in range(2):
                    x_buf[fs * r : fs * (r + 1), LANES * t : LANES * (t + 1)] = recv[
                        pl.ds(k * part + 2 * t + r, fs, stride=span), :
                    ]
            gram = share(0, k, dot(x_buf[...], x_buf[...], 1))
            mixed = three_steps(gram, one)
            for t in range(0, wide, 256):
                x3_buf[:, t : t + 256] = dot(mixed, x_buf[:, t : t + 256])
            gram = share(1, k, dot(x3_buf[...], x3_buf[...], 1))
            mixed = two_steps(gram, one)
            for t in range(cols):
                out = dot(mixed, x3_buf[:, LANES * t : LANES * (t + 1)])
                for r in range(2):
                    res[pl.ds(k * part + 2 * t + r, fs, stride=span), :] = out[fs * r : fs * (r + 1)]
            send_all(res, back, k, b_send, b_recv)
            back[block(k, me), :] = res[block(k, me), :]
            return carry

        lax.fori_loop(0, chunks, work, 0)
        pltpu.make_async_copy(weights, w_buf, w_sem).wait()

        def finish(k, carry):
            wait_rows(back, others, b_recv.at[k])
            new_w[chunk(k), :] = w_buf[chunk(k), :] - RATE * back[chunk(k), :]
            return carry

        lax.fori_loop(0, chunks, finish, 0)
        wait_rows(new_m, chunks * others, f_send)
        wait_rows(res, chunks * others, b_send)

    total = chunks * part
    buf = pltpu.VMEM((total, LANES), jnp.float32)
    scratch = [buf] * 6 + [
        pltpu.VMEM((SIDE, wide), jnp.float32),
        pltpu.VMEM((SIDE, wide), jnp.float32),
        pltpu.VMEM((2, chunks, tp, SIDE, SIDE), jnp.float32),
    ]
    dma = pltpu.SemaphoreType.DMA
    scratch += [
        dma((chunks,)), dma((chunks,)), dma,
        dma, dma((chunks,)), dma, dma((chunks,)), dma((2, tp - 1)), dma((2, chunks, tp - 1)),
    ]
    hbm = pl.BlockSpec(memory_space=pltpu.HBM)
    return pl.pallas_call(
        kernel,
        out_shape=[jax.ShapeDtypeStruct((total, LANES), jnp.float32)] * 2,
        in_specs=[hbm] * 3,
        out_specs=[pl.BlockSpec(memory_space=pltpu.VMEM)] * 2,
        scratch_shapes=scratch,
        compiler_params=pltpu.CompilerParams(
            collective_id=0, has_side_effects=True, vmem_limit_bytes=40 << 20
        ),
        name="step",
    )


def flat(a):
    m, r, w = a.shape
    return a.reshape(m, r, w // LANES, LANES).transpose(0, 2, 1, 3).reshape(-1, LANES)


def solution(mesh):
    fs, tp = mesh.shape["fsdp"], mesh.shape["tp"]

    def body(slopes_in, moments_in, weights_in):
        mats, rows, wide = slopes_in.shape

        def unflat(a):
            a = a.reshape(mats, wide // LANES, rows, LANES).transpose(0, 2, 1, 3)
            return a.reshape(mats, rows, wide)

        new_w, new_m = make_kernel(fs, tp, mats, wide)(
            flat(slopes_in), flat(moments_in), flat(weights_in)
        )
        return unflat(new_w), unflat(new_m)

    spec = P(None, "fsdp", "tp")
    return jax.shard_map(
        body, mesh=mesh, in_specs=(spec,) * 3, out_specs=(spec,) * 2, check_vma=False
    )
```

```python
import jax
import jax.numpy as jnp
from jax import lax
from jax.experimental import pallas as pl
from jax.experimental.pallas import tpu as pltpu
from jax.sharding import PartitionSpec as P

HOLD = 0.8
RATE = 1.0
CA, CB, CC = 3.4445, -4.775, 2.0315
LANES = 128
SIDE = 128
RING = 8
AROUND = (0, 1, 7, 2, 6, 3, 5, 4)
MESH = pl.DeviceIdType.MESH


def dot(a, b, contract=0):
    return lax.dot_general(
        a,
        b,
        (((1,), (contract,)), ((), ())),
        precision=lax.Precision.HIGHEST,
        preferred_element_type=jnp.float32,
    )


def eye():
    shape = (SIDE, SIDE)
    rows = lax.broadcasted_iota(jnp.int32, shape, 0)
    return (rows == lax.broadcasted_iota(jnp.int32, shape, 1)).astype(jnp.float32)


def poly(gram, one):
    return CA * one + CB * gram + CC * dot(gram, gram)


def three_steps(gram, one):
    scale = lax.rsqrt(jnp.sum(gram * one) + 1e-06)
    gram = gram * (scale * scale)
    first = poly(gram, one)
    gram = dot(dot(first, gram), first)
    second = poly(gram, one)
    both = dot(second, first)
    gram = dot(dot(second, gram), second)
    return dot(poly(gram, one), both) * scale


def two_steps(gram, one):
    first = poly(gram, one)
    gram = dot(dot(first, gram), first)
    return dot(poly(gram, one), first)


def make_kernel(fs, tp, mats, wide):
    chunks = mats // fs
    span = 2 * wide // LANES
    cols = wide // LANES
    part = fs * span
    others = fs - 1

    def kernel(
        slopes, moments, weights, new_w, new_m,
        s_buf, m_buf, recv, res, back, w_buf, x_buf, x3_buf, grams,
        s_sem, m_sem, w_sem, f_send, f_recv, b_send, b_recv, g_send, g_recv, ready,
    ):
        me = lax.axis_index("fsdp")
        col = lax.axis_index("tp")
        z, x, c = me // RING, (me // 2) % 4, me % 2

        rings = [(z + far) % RING * 8 for far in range(RING)]

        def peers(fars, visit):
            def at(n, carry):
                near = (x + n // 2) % 4 * 2 + (c + n % 2) % 2
                for far in fars:
                    visit(rings[far] + near)
                return carry

            if 0 in fars:
                for far in fars:
                    if far:
                        visit(rings[far] + x * 2 + c)
                lax.fori_loop(1, 8, at, 0)
            else:
                lax.fori_loop(0, 8, at, 0)

        def chunk(k):
            return pl.ds(pl.multiple_of(k * part, part), part)

        def block(k, j):
            return pl.ds(pl.multiple_of(k * part + j * span, span), span)

        def load(k):
            pltpu.make_async_copy(slopes.at[chunk(k)], s_buf.at[chunk(k)], s_sem.at[k]).start()
            pltpu.make_async_copy(moments.at[chunk(k)], m_buf.at[chunk(k)], m_sem.at[k]).start()

        def send_all(src, dst, k, send_sem, recv_sem, fars=AROUND):
            def send(j):
                pltpu.make_async_remote_copy(
                    src_ref=src.at[block(k, j)],
                    dst_ref=dst.at[block(k, me)],
                    send_sem=send_sem,
                    recv_sem=recv_sem.at[k],
                    device_id=(j, col),
                    device_id_type=MESH,
                ).start()

            peers(fars, send)

        def wait_rows(buf, n, sem):
            rows = pl.ds(0, n * span)
            pltpu.make_async_copy(buf.at[rows], buf.at[rows], sem).wait()

        load(0)
        barrier = pltpu.get_barrier_semaphore()

        def greet(j):
            pl.semaphore_signal(barrier, inc=1, device_id=(j, col), device_id_type=MESH)

        peers((1, 7, 0), greet)
        for d in range(1, tp):
            pl.semaphore_signal(barrier, inc=1, device_id=(me, (col + d) % tp), device_id_type=MESH)
        for k in range(1, chunks):
            load(k)
        pltpu.make_async_copy(weights, w_buf, w_sem).start()

        def momentum(k, carry):
            pltpu.make_async_copy(slopes.at[chunk(k)], s_buf.at[chunk(k)], s_sem.at[k]).wait()
            pltpu.make_async_copy(moments.at[chunk(k)], m_buf.at[chunk(k)], m_sem.at[k]).wait()
            new_m[chunk(k), :] = HOLD * m_buf[chunk(k), :] + s_buf[chunk(k), :]
            return carry

        def tell(turn):
            for far in (1, 7):
                pl.semaphore_signal(
                    ready.at[turn], inc=1, device_id=(rings[far] + x * 2 + c, col), device_id_type=MESH
                )

        pl.semaphore_wait(barrier, 3 * 8 - 1 + tp - 1)
        tell(0)
        momentum(0, 0)
        send_all(new_m, recv, 0, f_send, f_recv, (1, 7, 0))
        for turn, fars in enumerate(((2, 6), (3, 5), (4,))):
            pl.semaphore_wait(ready.at[turn], 2)
            if turn < 2:
                tell(turn + 1)
            send_all(new_m, recv, 0, f_send, f_recv, fars)
        recv[block(0, me), :] = new_m[block(0, me), :]

        def spread(k, carry):
            send_all(new_m, recv, k, f_send, f_recv)
            recv[block(k, me), :] = new_m[block(k, me), :]
            return carry

        def rest(k, carry):
            momentum(k, 0)
            return spread(k, 0)

        lax.fori_loop(1, chunks, rest, 0)

        one = eye()

        def shares(turn, k):
            return [
                pltpu.make_async_remote_copy(
                    src_ref=grams.at[turn, k, col],
                    dst_ref=grams.at[turn, k, col],
                    send_sem=g_send.at[turn, d - 1],
                    recv_sem=g_recv.at[turn, k, d - 1],
                    device_id=(me, (col + d) % tp),
                    device_id_type=MESH,
                )
                for d in range(1, tp)
            ]

        def share(turn, k, value):
            grams[turn, k, col] = value
            for copy in shares(turn, k):
                copy.start()

        def shared(turn, k):
            for copy in shares(turn, k):
                copy.wait()
            total = grams[turn, k, 0]
            for t in range(1, tp):
                total = total + grams[turn, k, t]
            return total

        def take(k):
            wait_rows(recv, others, f_recv.at[k])
            for t in range(cols):
                for r in range(2):
                    x_buf[fs * r : fs * (r + 1), LANES * t : LANES * (t + 1)] = recv[
                        pl.ds(k * part + 2 * t + r, fs, stride=span), :
                    ]
            share(0, k, dot(x_buf[...], x_buf[...], 1))

        def work(k, carry):
            mixed = three_steps(shared(0, k), one)
            for t in range(0, wide, 256):
                x3_buf[:, t : t + 256] = dot(mixed, x_buf[:, t : t + 256])
            share(1, k, dot(x3_buf[...], x3_buf[...], 1))

            @pl.when(k + 1 < chunks)
            def _():
                take(k + 1)

            mixed = two_steps(shared(1, k), one)
            for t in range(cols):
                out = dot(mixed, x3_buf[:, LANES * t : LANES * (t + 1)])
                for r in range(2):
                    res[pl.ds(k * part + 2 * t + r, fs, stride=span), :] = out[fs * r : fs * (r + 1)]
            send_all(res, back, k, b_send, b_recv)
            back[block(k, me), :] = res[block(k, me), :]
            return carry

        take(0)
        lax.fori_loop(0, chunks, work, 0)
        pltpu.make_async_copy(weights, w_buf, w_sem).wait()

        def finish(k, carry):
            wait_rows(back, others, b_recv.at[k])
            new_w[chunk(k), :] = w_buf[chunk(k), :] - RATE * back[chunk(k), :]
            return carry

        lax.fori_loop(0, chunks, finish, 0)
        wait_rows(new_m, chunks * others, f_send)
        wait_rows(res, chunks * others, b_send)

    total = chunks * part
    buf = pltpu.VMEM((total, LANES), jnp.float32)
    scratch = [buf] * 6 + [
        pltpu.VMEM((SIDE, wide), jnp.float32),
        pltpu.VMEM((SIDE, wide), jnp.float32),
        pltpu.VMEM((2, chunks, tp, SIDE, SIDE), jnp.float32),
    ]
    dma = pltpu.SemaphoreType.DMA
    scratch += [
        dma((chunks,)), dma((chunks,)), dma,
        dma, dma((chunks,)), dma, dma((chunks,)), dma((2, tp - 1)), dma((2, chunks, tp - 1)),
        pltpu.SemaphoreType.REGULAR((3,)),
    ]
    hbm = pl.BlockSpec(memory_space=pltpu.HBM)
    return pl.pallas_call(
        kernel,
        out_shape=[jax.ShapeDtypeStruct((total, LANES), jnp.float32)] * 2,
        in_specs=[hbm] * 3,
        out_specs=[pl.BlockSpec(memory_space=pltpu.VMEM)] * 2,
        scratch_shapes=scratch,
        compiler_params=pltpu.CompilerParams(
            collective_id=0, has_side_effects=True, vmem_limit_bytes=48 << 20
        ),
        name="step",
    )


def store(new_w, new_m):
    def kernel(w_in, m_in, w_out, m_out, sem):
        copies = [
            pltpu.make_async_copy(w_in, w_out, sem.at[0]),
            pltpu.make_async_copy(m_in, m_out, sem.at[1]),
        ]
        for copy in copies:
            copy.start()
        for copy in copies:
            copy.wait()

    return pl.pallas_call(
        kernel,
        out_shape=[jax.ShapeDtypeStruct(new_w.shape, new_w.dtype)] * 2,
        in_specs=[pl.BlockSpec(memory_space=pltpu.VMEM)] * 2,
        out_specs=[pl.BlockSpec(memory_space=pltpu.HBM)] * 2,
        scratch_shapes=[pltpu.SemaphoreType.DMA((2,))],
        compiler_params=pltpu.CompilerParams(vmem_limit_bytes=8 << 20),
        name="store",
    )(new_w, new_m)


def flat(a):
    m, r, w = a.shape
    return a.reshape(m, r, w // LANES, LANES).transpose(0, 2, 1, 3).reshape(-1, LANES)


def solution(mesh):
    fs, tp = mesh.shape["fsdp"], mesh.shape["tp"]

    def body(slopes_in, moments_in, weights_in):
        mats, rows, wide = slopes_in.shape

        def unflat(a):
            a = a.reshape(mats, wide // LANES, rows, LANES).transpose(0, 2, 1, 3)
            return a.reshape(mats, rows, wide)

        new_w, new_m = store(
            *make_kernel(fs, tp, mats, wide)(
                flat(slopes_in), flat(moments_in), flat(weights_in)
            )
        )
        return unflat(new_w), unflat(new_m)

    spec = P(None, "fsdp", "tp")
    return jax.shard_map(
        body, mesh=mesh, in_specs=(spec,) * 3, out_specs=(spec,) * 2, check_vma=False
    )
```

```python
import jax
import jax.numpy as jnp
from jax import lax
from jax.experimental import pallas as pl
from jax.experimental.pallas import tpu as pltpu
from jax.sharding import PartitionSpec as P

HOLD = 0.8
RATE = 1.0
CA, CB, CC = 3.4445, -4.775, 2.0315
LANES = 128
SIDE = 128
RING = 8
AROUND = (4, 3, 5, 2, 6, 1, 7, 0)
MESH = pl.DeviceIdType.MESH


def dot(a, b, contract=0):
    return lax.dot_general(
        a,
        b,
        (((1,), (contract,)), ((), ())),
        precision=lax.Precision.HIGHEST,
        preferred_element_type=jnp.float32,
    )


def eye():
    shape = (SIDE, SIDE)
    rows = lax.broadcasted_iota(jnp.int32, shape, 0)
    return (rows == lax.broadcasted_iota(jnp.int32, shape, 1)).astype(jnp.float32)


def poly(gram, one):
    return CA * one + CB * gram + CC * dot(gram, gram)


def three_steps(gram, one):
    scale = lax.rsqrt(jnp.sum(gram * one) + 1e-06)
    gram = gram * (scale * scale)
    first = poly(gram, one)
    gram = dot(dot(first, gram), first)
    second = poly(gram, one)
    both = dot(second, first)
    gram = dot(dot(second, gram), second)
    return dot(poly(gram, one), both) * scale


def two_steps(gram, one):
    first = poly(gram, one)
    gram = dot(dot(first, gram), first)
    return dot(poly(gram, one), first)


def make_kernel(fs, tp, mats, wide):
    chunks = mats // fs
    span = 2 * wide // LANES
    cols = wide // LANES
    part = fs * span
    others = fs - 1

    def kernel(
        slopes, moments, weights, new_w, new_m,
        s_buf, m_buf, recv, res, back, w_buf, x_buf, x3_buf, grams,
        s_sem, m_sem, w_sem, f_send, f_recv, b_send, b_recv, g_send, g_recv, ready,
    ):
        me = lax.axis_index("fsdp")
        col = lax.axis_index("tp")
        z, x, c = me // RING, (me // 2) % 4, me % 2

        rings = [(z + far) % RING * 8 for far in range(RING)]

        def peers(fars, visit):
            def at(n, carry):
                n = 8 - n
                near = (x + n // 2) % 4 * 2 + (c + n % 2) % 2
                for far in fars:
                    visit(rings[far] + near)
                return carry

            if 0 in fars:
                lax.fori_loop(1, 8, at, 0)
                for far in fars:
                    if far:
                        visit(rings[far] + x * 2 + c)
            else:
                lax.fori_loop(0, 8, at, 0)

        def chunk(k):
            return pl.ds(pl.multiple_of(k * part, part), part)

        def block(k, j):
            return pl.ds(pl.multiple_of(k * part + j * span, span), span)

        def load(k):
            pltpu.make_async_copy(slopes.at[chunk(k)], s_buf.at[chunk(k)], s_sem.at[k]).start()
            pltpu.make_async_copy(moments.at[chunk(k)], m_buf.at[chunk(k)], m_sem.at[k]).start()

        def send_all(src, dst, k, send_sem, recv_sem, fars=AROUND):
            def send(j):
                pltpu.make_async_remote_copy(
                    src_ref=src.at[block(k, j)],
                    dst_ref=dst.at[block(k, me)],
                    send_sem=send_sem,
                    recv_sem=recv_sem.at[k],
                    device_id=(j, col),
                    device_id_type=MESH,
                ).start()

            peers(fars, send)

        def wait_rows(buf, n, sem):
            rows = pl.ds(0, n * span)
            pltpu.make_async_copy(buf.at[rows], buf.at[rows], sem).wait()

        load(0)
        barrier = pltpu.get_barrier_semaphore()

        def greet(j):
            pl.semaphore_signal(barrier, inc=1, device_id=(j, col), device_id_type=MESH)

        peers((1, 7, 0), greet)
        for d in range(1, tp):
            pl.semaphore_signal(barrier, inc=1, device_id=(me, (col + d) % tp), device_id_type=MESH)
        for k in range(1, chunks):
            load(k)
        pltpu.make_async_copy(weights, w_buf, w_sem).start()

        def momentum(k, carry):
            pltpu.make_async_copy(slopes.at[chunk(k)], s_buf.at[chunk(k)], s_sem.at[k]).wait()
            pltpu.make_async_copy(moments.at[chunk(k)], m_buf.at[chunk(k)], m_sem.at[k]).wait()
            new_m[chunk(k), :] = HOLD * m_buf[chunk(k), :] + s_buf[chunk(k), :]
            return carry

        def tell(turn):
            for far in (1, 7):
                pl.semaphore_signal(
                    ready.at[turn], inc=1, device_id=(rings[far] + x * 2 + c, col), device_id_type=MESH
                )

        pl.semaphore_wait(barrier, 3 * 8 - 1 + tp - 1)
        tell(0)
        momentum(0, 0)
        send_all(new_m, recv, 0, f_send, f_recv, (1, 7, 0))
        for turn, fars in enumerate(((2, 6), (3, 5), (4,))):
            pl.semaphore_wait(ready.at[turn], 2)
            if turn < 2:
                tell(turn + 1)
            send_all(new_m, recv, 0, f_send, f_recv, fars)
        recv[block(0, me), :] = new_m[block(0, me), :]

        def spread(k, carry):
            send_all(new_m, recv, k, f_send, f_recv)
            recv[block(k, me), :] = new_m[block(k, me), :]
            return carry

        def rest(k, carry):
            momentum(k, 0)
            return spread(k, 0)

        lax.fori_loop(1, chunks, rest, 0)

        one = eye()

        def shares(turn, k):
            return [
                pltpu.make_async_remote_copy(
                    src_ref=grams.at[turn, k, col],
                    dst_ref=grams.at[turn, k, col],
                    send_sem=g_send.at[turn, d - 1],
                    recv_sem=g_recv.at[turn, k, d - 1],
                    device_id=(me, (col + d) % tp),
                    device_id_type=MESH,
                )
                for d in range(1, tp)
            ]

        def share(turn, k, value):
            grams[turn, k, col] = value
            for copy in shares(turn, k):
                copy.start()

        def shared(turn, k):
            for copy in shares(turn, k):
                copy.wait()
            total = grams[turn, k, 0]
            for t in range(1, tp):
                total = total + grams[turn, k, t]
            return total

        def take(k):
            wait_rows(recv, others, f_recv.at[k])
            for t in range(cols):
                for r in range(2):
                    x_buf[fs * r : fs * (r + 1), LANES * t : LANES * (t + 1)] = recv[
                        pl.ds(k * part + 2 * t + r, fs, stride=span), :
                    ]
            share(0, k, dot(x_buf[...], x_buf[...], 1))

        def work(k, carry):
            mixed = three_steps(shared(0, k), one)
            for t in range(0, wide, 256):
                x3_buf[:, t : t + 256] = dot(mixed, x_buf[:, t : t + 256])
            share(1, k, dot(x3_buf[...], x3_buf[...], 1))

            @pl.when(k + 1 < chunks)
            def _():
                take(k + 1)

            mixed = two_steps(shared(1, k), one)
            for t in range(cols):
                out = dot(mixed, x3_buf[:, LANES * t : LANES * (t + 1)])
                for r in range(2):
                    res[pl.ds(k * part + 2 * t + r, fs, stride=span), :] = out[fs * r : fs * (r + 1)]
            send_all(res, back, k, b_send, b_recv)
            back[block(k, me), :] = res[block(k, me), :]
            return carry

        take(0)
        lax.fori_loop(0, chunks, work, 0)
        pltpu.make_async_copy(weights, w_buf, w_sem).wait()

        def finish(k, carry):
            wait_rows(back, others, b_recv.at[k])
            new_w[chunk(k), :] = w_buf[chunk(k), :] - RATE * back[chunk(k), :]
            return carry

        lax.fori_loop(0, chunks, finish, 0)
        wait_rows(new_m, chunks * others, f_send)
        wait_rows(res, chunks * others, b_send)

    total = chunks * part
    buf = pltpu.VMEM((total, LANES), jnp.float32)
    strided = pltpu.VMEM((total + span, LANES), jnp.float32)
    scratch = [buf] * 2 + [strided] * 2 + [buf] * 2 + [
        pltpu.VMEM((SIDE, wide), jnp.float32),
        pltpu.VMEM((SIDE, wide), jnp.float32),
        pltpu.VMEM((2, chunks, tp, SIDE, SIDE), jnp.float32),
    ]
    dma = pltpu.SemaphoreType.DMA
    scratch += [
        dma((chunks,)), dma((chunks,)), dma,
        dma, dma((chunks,)), dma, dma((chunks,)), dma((2, tp - 1)), dma((2, chunks, tp - 1)),
        pltpu.SemaphoreType.REGULAR((3,)),
    ]
    hbm = pl.BlockSpec(memory_space=pltpu.HBM)
    return pl.pallas_call(
        kernel,
        out_shape=[jax.ShapeDtypeStruct((total, LANES), jnp.float32)] * 2,
        in_specs=[hbm] * 3,
        out_specs=[pl.BlockSpec(memory_space=pltpu.VMEM)] * 2,
        scratch_shapes=scratch,
        compiler_params=pltpu.CompilerParams(
            collective_id=0, has_side_effects=True, vmem_limit_bytes=48 << 20
        ),
        name="step",
    )


def store(new_w, new_m):
    def kernel(w_in, m_in, w_out, m_out, sem):
        copies = [
            pltpu.make_async_copy(w_in, w_out, sem.at[0]),
            pltpu.make_async_copy(m_in, m_out, sem.at[1]),
        ]
        for copy in copies:
            copy.start()
        for copy in copies:
            copy.wait()

    return pl.pallas_call(
        kernel,
        out_shape=[jax.ShapeDtypeStruct(new_w.shape, new_w.dtype)] * 2,
        in_specs=[pl.BlockSpec(memory_space=pltpu.VMEM)] * 2,
        out_specs=[pl.BlockSpec(memory_space=pltpu.HBM)] * 2,
        scratch_shapes=[pltpu.SemaphoreType.DMA((2,))],
        compiler_params=pltpu.CompilerParams(vmem_limit_bytes=8 << 20),
        name="store",
    )(new_w, new_m)


def flat(a):
    m, r, w = a.shape
    return a.reshape(m, r, w // LANES, LANES).transpose(0, 2, 1, 3).reshape(-1, LANES)


def solution(mesh):
    fs, tp = mesh.shape["fsdp"], mesh.shape["tp"]

    def body(slopes_in, moments_in, weights_in):
        mats, rows, wide = slopes_in.shape

        def unflat(a):
            a = a.reshape(mats, wide // LANES, rows, LANES).transpose(0, 2, 1, 3)
            return a.reshape(mats, rows, wide)

        new_w, new_m = store(
            *make_kernel(fs, tp, mats, wide)(
                flat(slopes_in), flat(moments_in), flat(weights_in)
            )
        )
        return unflat(new_w), unflat(new_m)

    spec = P(None, "fsdp", "tp")
    return jax.shard_map(
        body, mesh=mesh, in_specs=(spec,) * 3, out_specs=(spec,) * 2, check_vma=False
    )
```

```python
import jax
import jax.numpy as jnp
from jax import lax
from jax.experimental import pallas as pl
from jax.experimental.pallas import tpu as pltpu
from jax.sharding import PartitionSpec as P

HOLD = 0.8
RATE = 1.0
CA, CB, CC = 3.4445, -4.775, 2.0315
LANES = 128
SIDE = 128
RING = 8
AROUND = (4, 3, 5, 2, 6, 1, 7, 0)
MESH = pl.DeviceIdType.MESH


def dot(a, b, contract=0):
    return lax.dot_general(
        a,
        b,
        (((1,), (contract,)), ((), ())),
        precision=lax.Precision.HIGHEST,
        preferred_element_type=jnp.float32,
    )


def eye():
    shape = (SIDE, SIDE)
    rows = lax.broadcasted_iota(jnp.int32, shape, 0)
    return (rows == lax.broadcasted_iota(jnp.int32, shape, 1)).astype(jnp.float32)


def poly(gram, one):
    return CA * one + CB * gram + CC * dot(gram, gram)


def three_steps(gram, one):
    scale = lax.rsqrt(jnp.sum(gram * one) + 1e-06)
    gram = gram * (scale * scale)
    first = poly(gram, one)
    gram = dot(dot(first, gram), first)
    second = poly(gram, one)
    both = dot(second, first)
    gram = dot(dot(second, gram), second)
    return dot(poly(gram, one), both) * scale


def two_steps(gram, one):
    first = poly(gram, one)
    gram = dot(dot(first, gram), first)
    return dot(poly(gram, one), first)


def make_kernel(fs, tp, mats, wide):
    chunks = mats // fs
    span = 2 * wide // LANES
    cols = wide // LANES
    part = fs * span
    others = fs - 1

    def kernel(
        slopes, moments, weights, new_w, new_m,
        s_buf, m_buf, recv, res, back, w_buf, x_buf, x3_buf, grams,
        s_sem, m_sem, w_sem, f_send, f_recv, b_send, b_recv, g_send, g_recv, ready,
    ):
        me = lax.axis_index("fsdp")
        col = lax.axis_index("tp")
        z, x, c = me // RING, (me // 2) % 4, me % 2

        rings = [(z + far) % RING * 8 for far in range(RING)]

        def peers(fars, visit):
            def at(n, carry):
                n = 8 - n
                near = (x + n // 2) % 4 * 2 + (c + n % 2) % 2
                for far in fars:
                    visit(rings[far] + near)
                return carry

            if 0 in fars:
                lax.fori_loop(1, 8, at, 0)
                for far in fars:
                    if far:
                        visit(rings[far] + x * 2 + c)
            else:
                lax.fori_loop(0, 8, at, 0)

        def chunk(k):
            return pl.ds(pl.multiple_of(k * part, part), part)

        def block(k, j):
            return pl.ds(pl.multiple_of(k * part + j * span, span), span)

        def load(k):
            pltpu.make_async_copy(slopes.at[chunk(k)], s_buf.at[chunk(k)], s_sem.at[k]).start()
            pltpu.make_async_copy(moments.at[chunk(k)], m_buf.at[chunk(k)], m_sem.at[k]).start()

        def send_all(src, dst, k, send_sem, recv_sem, fars=AROUND):
            def send(j):
                pltpu.make_async_remote_copy(
                    src_ref=src.at[block(k, j)],
                    dst_ref=dst.at[block(k, me)],
                    send_sem=send_sem,
                    recv_sem=recv_sem.at[k],
                    device_id=(j, col),
                    device_id_type=MESH,
                ).start()

            peers(fars, send)

        def send_last(k, zs):
            def at(n, carry):
                n = 8 - n
                near = (x + n // 2) % 4 * 2 + (c + n % 2) % 2
                for to in zs:
                    j = to * 8 + near

                    @pl.when(j != me)
                    def _():
                        pltpu.make_async_remote_copy(
                            src_ref=res.at[block(k, j)],
                            dst_ref=back.at[block(k, me)],
                            send_sem=b_send,
                            recv_sem=b_recv.at[k],
                            device_id=(j, col),
                            device_id_type=MESH,
                        ).start()

                return carry

            lax.fori_loop(1, 9, at, 0)

        def wait_rows(buf, n, sem):
            rows = pl.ds(0, n * span)
            pltpu.make_async_copy(buf.at[rows], buf.at[rows], sem).wait()

        load(0)
        barrier = pltpu.get_barrier_semaphore()

        def greet(j):
            pl.semaphore_signal(barrier, inc=1, device_id=(j, col), device_id_type=MESH)

        peers((1, 7, 0), greet)
        for d in range(1, tp):
            pl.semaphore_signal(barrier, inc=1, device_id=(me, (col + d) % tp), device_id_type=MESH)
        for k in range(1, chunks):
            load(k)
        pltpu.make_async_copy(weights, w_buf, w_sem).start()

        def momentum(k, carry):
            pltpu.make_async_copy(slopes.at[chunk(k)], s_buf.at[chunk(k)], s_sem.at[k]).wait()
            pltpu.make_async_copy(moments.at[chunk(k)], m_buf.at[chunk(k)], m_sem.at[k]).wait()
            new_m[chunk(k), :] = HOLD * m_buf[chunk(k), :] + s_buf[chunk(k), :]
            return carry

        def tell(turn):
            for far in (1, 7):
                pl.semaphore_signal(
                    ready.at[turn], inc=1, device_id=(rings[far] + x * 2 + c, col), device_id_type=MESH
                )

        pl.semaphore_wait(barrier, 3 * 8 - 1 + tp - 1)
        tell(0)
        momentum(0, 0)
        send_all(new_m, recv, 0, f_send, f_recv, (1, 7, 0))
        for turn, fars in enumerate(((2, 6), (3, 5), (4,))):
            pl.semaphore_wait(ready.at[turn], 2)
            if turn < 2:
                tell(turn + 1)
            send_all(new_m, recv, 0, f_send, f_recv, fars)
        recv[block(0, me), :] = new_m[block(0, me), :]

        def spread(k, carry):
            send_all(new_m, recv, k, f_send, f_recv)
            recv[block(k, me), :] = new_m[block(k, me), :]
            return carry

        def rest(k, carry):
            momentum(k, 0)
            return spread(k, 0)

        lax.fori_loop(1, chunks, rest, 0)

        one = eye()

        def shares(turn, k):
            return [
                pltpu.make_async_remote_copy(
                    src_ref=grams.at[turn, k, col],
                    dst_ref=grams.at[turn, k, col],
                    send_sem=g_send.at[turn, d - 1],
                    recv_sem=g_recv.at[turn, k, d - 1],
                    device_id=(me, (col + d) % tp),
                    device_id_type=MESH,
                )
                for d in range(1, tp)
            ]

        def share(turn, k, value):
            grams[turn, k, col] = value
            for copy in shares(turn, k):
                copy.start()

        def shared(turn, k):
            for copy in shares(turn, k):
                copy.wait()
            total = grams[turn, k, 0]
            for t in range(1, tp):
                total = total + grams[turn, k, t]
            return total

        def take(k):
            wait_rows(recv, others, f_recv.at[k])
            for t in range(cols):
                for r in range(2):
                    x_buf[fs * r : fs * (r + 1), LANES * t : LANES * (t + 1)] = recv[
                        pl.ds(k * part + 2 * t + r, fs, stride=span), :
                    ]
            share(0, k, dot(x_buf[...], x_buf[...], 1))

        def work(k, carry):
            mixed = three_steps(shared(0, k), one)
            for t in range(0, wide, 256):
                x3_buf[:, t : t + 256] = dot(mixed, x_buf[:, t : t + 256])
            share(1, k, dot(x3_buf[...], x3_buf[...], 1))

            @pl.when(k + 1 < chunks)
            def _():
                take(k + 1)

            mixed = two_steps(shared(1, k), one)
            for t in range(cols):
                out = dot(mixed, x3_buf[:, LANES * t : LANES * (t + 1)])
                for r in range(2):
                    res[pl.ds(k * part + 2 * t + r, fs, stride=span), :] = out[fs * r : fs * (r + 1)]
            @pl.when(k + 1 < chunks)
            def _():
                send_all(res, back, k, b_send, b_recv)

            @pl.when(k + 1 == chunks)
            def _():
                send_last(k, (0, 1))
                send_last(k, (2, 3, 7, 4, 6, 5))

            back[block(k, me), :] = res[block(k, me), :]
            return carry

        take(0)
        lax.fori_loop(0, chunks, work, 0)
        pltpu.make_async_copy(weights, w_buf, w_sem).wait()

        def finish(k, carry):
            wait_rows(back, others, b_recv.at[k])
            new_w[chunk(k), :] = w_buf[chunk(k), :] - RATE * back[chunk(k), :]
            return carry

        lax.fori_loop(0, chunks, finish, 0)
        wait_rows(new_m, chunks * others, f_send)
        wait_rows(res, chunks * others, b_send)

    total = chunks * part
    buf = pltpu.VMEM((total, LANES), jnp.float32)
    strided = pltpu.VMEM((total + span, LANES), jnp.float32)
    scratch = [buf] * 2 + [strided] * 2 + [buf] * 2 + [
        pltpu.VMEM((SIDE, wide), jnp.float32),
        pltpu.VMEM((SIDE, wide), jnp.float32),
        pltpu.VMEM((2, chunks, tp, SIDE, SIDE), jnp.float32),
    ]
    dma = pltpu.SemaphoreType.DMA
    scratch += [
        dma((chunks,)), dma((chunks,)), dma,
        dma, dma((chunks,)), dma, dma((chunks,)), dma((2, tp - 1)), dma((2, chunks, tp - 1)),
        pltpu.SemaphoreType.REGULAR((3,)),
    ]
    hbm = pl.BlockSpec(memory_space=pltpu.HBM)
    return pl.pallas_call(
        kernel,
        out_shape=[jax.ShapeDtypeStruct((total, LANES), jnp.float32)] * 2,
        in_specs=[hbm] * 3,
        out_specs=[pl.BlockSpec(memory_space=pltpu.VMEM)] * 2,
        scratch_shapes=scratch,
        compiler_params=pltpu.CompilerParams(
            collective_id=0, has_side_effects=True, vmem_limit_bytes=48 << 20
        ),
        name="step",
    )


def store(new_w, new_m):
    def kernel(w_in, m_in, w_out, m_out, sem):
        copies = [
            pltpu.make_async_copy(w_in, w_out, sem.at[0]),
            pltpu.make_async_copy(m_in, m_out, sem.at[1]),
        ]
        for copy in copies:
            copy.start()
        for copy in copies:
            copy.wait()

    return pl.pallas_call(
        kernel,
        out_shape=[jax.ShapeDtypeStruct(new_w.shape, new_w.dtype)] * 2,
        in_specs=[pl.BlockSpec(memory_space=pltpu.VMEM)] * 2,
        out_specs=[pl.BlockSpec(memory_space=pltpu.HBM)] * 2,
        scratch_shapes=[pltpu.SemaphoreType.DMA((2,))],
        compiler_params=pltpu.CompilerParams(vmem_limit_bytes=8 << 20),
        name="store",
    )(new_w, new_m)


def flat(a):
    m, r, w = a.shape
    return a.reshape(m, r, w // LANES, LANES).transpose(0, 2, 1, 3).reshape(-1, LANES)


def solution(mesh):
    fs, tp = mesh.shape["fsdp"], mesh.shape["tp"]

    def body(slopes_in, moments_in, weights_in):
        mats, rows, wide = slopes_in.shape

        def unflat(a):
            a = a.reshape(mats, wide // LANES, rows, LANES).transpose(0, 2, 1, 3)
            return a.reshape(mats, rows, wide)

        new_w, new_m = store(
            *make_kernel(fs, tp, mats, wide)(
                flat(slopes_in), flat(moments_in), flat(weights_in)
            )
        )
        return unflat(new_w), unflat(new_m)

    spec = P(None, "fsdp", "tp")
    return jax.shard_map(
        body, mesh=mesh, in_specs=(spec,) * 3, out_specs=(spec,) * 2, check_vma=False
    )
```

```python
import jax
import jax.numpy as jnp
from jax import lax
from jax.experimental import pallas as pl
from jax.experimental.pallas import tpu as pltpu
from jax.sharding import PartitionSpec as P

HOLD = 0.8
RATE = 1.0
CA, CB, CC = 3.4445, -4.775, 2.0315
LANES = 128
SIDE = 128
RING = 8
AROUND = (4, 3, 5, 2, 6, 1, 7, 0)
MESH = pl.DeviceIdType.MESH


def dot(a, b, contract=0):
    return lax.dot_general(
        a,
        b,
        (((1,), (contract,)), ((), ())),
        precision=lax.Precision.HIGHEST,
        preferred_element_type=jnp.float32,
    )


def eye():
    shape = (SIDE, SIDE)
    rows = lax.broadcasted_iota(jnp.int32, shape, 0)
    return (rows == lax.broadcasted_iota(jnp.int32, shape, 1)).astype(jnp.float32)


def poly(gram, one):
    return CA * one + CB * gram + CC * dot(gram, gram)


def three_steps(gram, one):
    scale = lax.rsqrt(jnp.sum(gram * one) + 1e-06)
    gram = gram * (scale * scale)
    first = poly(gram, one)
    gram = dot(dot(first, gram), first)
    second = poly(gram, one)
    both = dot(second, first)
    gram = dot(dot(second, gram), second)
    return dot(poly(gram, one), both) * scale


def two_steps(gram, one):
    first = poly(gram, one)
    gram = dot(dot(first, gram), first)
    return dot(poly(gram, one), first)


def make_kernel(fs, tp, mats, wide):
    chunks = mats // fs
    span = 2 * wide // LANES
    cols = wide // LANES
    part = fs * span
    others = fs - 1

    def kernel(
        slopes, moments, weights, new_w, new_m,
        s_buf, m_buf, recv, res, back, w_buf, x_buf, x3_buf, grams,
        s_sem, m_sem, w_sem, f_send, f_recv, b_send, b_recv, g_send, g_recv, ready,
    ):
        me = lax.axis_index("fsdp")
        col = lax.axis_index("tp")
        z, x, c = me // RING, (me // 2) % 4, me % 2

        rings = [(z + far) % RING * 8 for far in range(RING)]

        def peers(fars, visit):
            def at(n, carry):
                n = 8 - n
                near = (x + n // 2) % 4 * 2 + (c + n % 2) % 2
                for far in fars:
                    visit(rings[far] + near)
                return carry

            if 0 in fars:
                lax.fori_loop(1, 8, at, 0)
                for far in fars:
                    if far:
                        visit(rings[far] + x * 2 + c)
            else:
                lax.fori_loop(0, 8, at, 0)

        def chunk(k):
            return pl.ds(pl.multiple_of(k * part, part), part)

        def block(k, j):
            return pl.ds(pl.multiple_of(k * part + j * span, span), span)

        def load(k):
            pltpu.make_async_copy(slopes.at[chunk(k)], s_buf.at[chunk(k)], s_sem.at[k]).start()
            pltpu.make_async_copy(moments.at[chunk(k)], m_buf.at[chunk(k)], m_sem.at[k]).start()

        def send_all(src, dst, k, send_sem, recv_sem, fars=AROUND):
            def send(j):
                pltpu.make_async_remote_copy(
                    src_ref=src.at[block(k, j)],
                    dst_ref=dst.at[block(k, me)],
                    send_sem=send_sem,
                    recv_sem=recv_sem.at[k],
                    device_id=(j, col),
                    device_id_type=MESH,
                ).start()

            peers(fars, send)

        def send_last(k, zs):
            def at(n, carry):
                n = 8 - n
                near = (x + n // 2) % 4 * 2 + (c + n % 2) % 2
                for to in zs:
                    j = to * 8 + near

                    @pl.when(j != me)
                    def _():
                        pltpu.make_async_remote_copy(
                            src_ref=res.at[block(k, j)],
                            dst_ref=back.at[block(k, me)],
                            send_sem=b_send,
                            recv_sem=b_recv.at[k],
                            device_id=(j, col),
                            device_id_type=MESH,
                        ).start()

                return carry

            lax.fori_loop(1, 9, at, 0)

        def wait_rows(buf, n, sem):
            rows = pl.ds(0, n * span)
            pltpu.make_async_copy(buf.at[rows], buf.at[rows], sem).wait()

        load(0)
        barrier = pltpu.get_barrier_semaphore()

        def greet(j):
            pl.semaphore_signal(barrier, inc=1, device_id=(j, col), device_id_type=MESH)

        peers((1, 7, 0), greet)
        for d in range(1, tp):
            pl.semaphore_signal(barrier, inc=1, device_id=(me, (col + d) % tp), device_id_type=MESH)
        for k in range(1, chunks):
            load(k)
        pltpu.make_async_copy(weights, w_buf, w_sem).start()

        def momentum(k, carry):
            pltpu.make_async_copy(slopes.at[chunk(k)], s_buf.at[chunk(k)], s_sem.at[k]).wait()
            pltpu.make_async_copy(moments.at[chunk(k)], m_buf.at[chunk(k)], m_sem.at[k]).wait()
            new_m[chunk(k), :] = HOLD * m_buf[chunk(k), :] + s_buf[chunk(k), :]
            return carry

        def tell(turn):
            for far in (1, 7):
                pl.semaphore_signal(
                    ready.at[turn], inc=1, device_id=(rings[far] + x * 2 + c, col), device_id_type=MESH
                )

        pl.semaphore_wait(barrier, 3 * 8 - 1 + tp - 1)
        tell(0)
        momentum(0, 0)
        send_all(new_m, recv, 0, f_send, f_recv, (1, 7, 0))
        for turn, fars in enumerate(((2, 6), (3, 5), (4,))):
            pl.semaphore_wait(ready.at[turn], 2)
            if turn < 2:
                tell(turn + 1)
            send_all(new_m, recv, 0, f_send, f_recv, fars)
        recv[block(0, me), :] = new_m[block(0, me), :]

        def spread(k, carry):
            send_all(new_m, recv, k, f_send, f_recv)
            recv[block(k, me), :] = new_m[block(k, me), :]
            return carry

        def rest(k, carry):
            momentum(k, 0)
            return spread(k, 0)

        lax.fori_loop(1, chunks, rest, 0)

        one = eye()

        def shares(turn, k):
            return [
                pltpu.make_async_remote_copy(
                    src_ref=grams.at[turn, k, col],
                    dst_ref=grams.at[turn, k, col],
                    send_sem=g_send.at[turn, d - 1],
                    recv_sem=g_recv.at[turn, k, d - 1],
                    device_id=(me, (col + d) % tp),
                    device_id_type=MESH,
                )
                for d in range(1, tp)
            ]

        def share(turn, k, value):
            grams[turn, k, col] = value
            for copy in shares(turn, k):
                copy.start()

        def shared(turn, k):
            for copy in shares(turn, k):
                copy.wait()
            total = grams[turn, k, 0]
            for t in range(1, tp):
                total = total + grams[turn, k, t]
            return total

        def take(k):
            wait_rows(recv, others, f_recv.at[k])
            for t in range(cols):
                for r in range(2):
                    x_buf[fs * r : fs * (r + 1), LANES * t : LANES * (t + 1)] = recv[
                        pl.ds(k * part + 2 * t + r, fs, stride=span), :
                    ]
            share(0, k, dot(x_buf[...], x_buf[...], 1))

        def work(k, carry):
            mixed = three_steps(shared(0, k), one)
            for t in range(0, wide, 256):
                x3_buf[:, t : t + 256] = dot(mixed, x_buf[:, t : t + 256])
            share(1, k, dot(x3_buf[...], x3_buf[...], 1))

            @pl.when(k + 1 < chunks)
            def _():
                take(k + 1)

            mixed = two_steps(shared(1, k), one)
            for t in range(cols):
                out = dot(mixed, x3_buf[:, LANES * t : LANES * (t + 1)])
                for r in range(2):
                    res[pl.ds(k * part + 2 * t + r, fs, stride=span), :] = out[fs * r : fs * (r + 1)]
            @pl.when(k + 1 < chunks)
            def _():
                send_all(res, back, k, b_send, b_recv)

            @pl.when(k + 1 == chunks)
            def _():
                send_last(k, (2, 0, 1))
                send_last(k, (3, 7, 4, 6, 5))

            back[block(k, me), :] = res[block(k, me), :]
            return carry

        take(0)
        lax.fori_loop(0, chunks, work, 0)
        pltpu.make_async_copy(weights, w_buf, w_sem).wait()

        def finish(k, carry):
            wait_rows(back, others, b_recv.at[k])
            new_w[chunk(k), :] = w_buf[chunk(k), :] - RATE * back[chunk(k), :]
            return carry

        lax.fori_loop(0, chunks, finish, 0)
        wait_rows(new_m, chunks * others, f_send)
        wait_rows(res, chunks * others, b_send)

    total = chunks * part
    buf = pltpu.VMEM((total, LANES), jnp.float32)
    strided = pltpu.VMEM((total + span, LANES), jnp.float32)
    scratch = [buf] * 2 + [strided] * 2 + [buf] * 2 + [
        pltpu.VMEM((SIDE, wide), jnp.float32),
        pltpu.VMEM((SIDE, wide), jnp.float32),
        pltpu.VMEM((2, chunks, tp, SIDE, SIDE), jnp.float32),
    ]
    dma = pltpu.SemaphoreType.DMA
    scratch += [
        dma((chunks,)), dma((chunks,)), dma,
        dma, dma((chunks,)), dma, dma((chunks,)), dma((2, tp - 1)), dma((2, chunks, tp - 1)),
        pltpu.SemaphoreType.REGULAR((3,)),
    ]
    hbm = pl.BlockSpec(memory_space=pltpu.HBM)
    return pl.pallas_call(
        kernel,
        out_shape=[jax.ShapeDtypeStruct((total, LANES), jnp.float32)] * 2,
        in_specs=[hbm] * 3,
        out_specs=[pl.BlockSpec(memory_space=pltpu.VMEM)] * 2,
        scratch_shapes=scratch,
        compiler_params=pltpu.CompilerParams(
            collective_id=0, has_side_effects=True, vmem_limit_bytes=48 << 20
        ),
        name="step",
    )


def store(new_w, new_m):
    def kernel(w_in, m_in, w_out, m_out, sem):
        copies = [
            pltpu.make_async_copy(w_in, w_out, sem.at[0]),
            pltpu.make_async_copy(m_in, m_out, sem.at[1]),
        ]
        for copy in copies:
            copy.start()
        for copy in copies:
            copy.wait()

    return pl.pallas_call(
        kernel,
        out_shape=[jax.ShapeDtypeStruct(new_w.shape, new_w.dtype)] * 2,
        in_specs=[pl.BlockSpec(memory_space=pltpu.VMEM)] * 2,
        out_specs=[pl.BlockSpec(memory_space=pltpu.HBM)] * 2,
        scratch_shapes=[pltpu.SemaphoreType.DMA((2,))],
        compiler_params=pltpu.CompilerParams(vmem_limit_bytes=8 << 20),
        name="store",
    )(new_w, new_m)


def flat(a):
    m, r, w = a.shape
    return a.reshape(m, r, w // LANES, LANES).transpose(0, 2, 1, 3).reshape(-1, LANES)


def solution(mesh):
    fs, tp = mesh.shape["fsdp"], mesh.shape["tp"]

    def body(slopes_in, moments_in, weights_in):
        mats, rows, wide = slopes_in.shape

        def unflat(a):
            a = a.reshape(mats, wide // LANES, rows, LANES).transpose(0, 2, 1, 3)
            return a.reshape(mats, rows, wide)

        new_w, new_m = store(
            *make_kernel(fs, tp, mats, wide)(
                flat(slopes_in), flat(moments_in), flat(weights_in)
            )
        )
        return unflat(new_w), unflat(new_m)

    spec = P(None, "fsdp", "tp")
    return jax.shard_map(
        body, mesh=mesh, in_specs=(spec,) * 3, out_specs=(spec,) * 2, check_vma=False
    )
```
